128 devices in a mesh: blk: 64 (over x_lo, y, z, core), tensor: 2 (over x_hi).
Axes of the slice: x: 4 (x_hi: 2, x_lo: 2; x = x_hi * 2 + x_lo), y: 4, z: 4, core: 2. Of those that a mesh axis runs over, the one named last changes fastest.
Arguments:
- tokens: bfloat16 [256, 8192], P('blk'), may hold values from -6 to 6
- gate_weight: bfloat16 [29568, 8192], P(('blk', 'tensor')), may hold values from -0.0625 to 0.0625
- up_weight: bfloat16 [29568, 8192], P(('blk', 'tensor')), may hold values from -0.0625 to 0.0625
- down_weight: bfloat16 [29568, 8192], P(('blk', 'tensor')), may hold values from -0.03125 to 0.03125
Outputs:
- mixed: bfloat16 [256, 8192], P(('blk', 'tensor'))
The draws below stay inside these ranges and needn't reach their ends.
All inputs are finite; a program needn't handle non-finite values.
Results may differ from the reference program's by a relative error of at most 0.009.
Values may be sent and summed in bfloat16 or wider, within the bound.
No kernel may reach another device: no remote copies, remote signals or barrier semaphores. Data moves between devices by JAX's collectives and lax.ppermute only.
A program may use at most 64 MiB of HBM per device.

```python
import jax
import jax.numpy as jnp

D = 8192
FF = 29568
TOKENS = 256


def level_of(own_key, extent, shards, low, high):
    factor_of, own = 1.0, jax.random.fold_in(own_key, 6)
    for axis_at, shards_of in shards:
        draws = jnp.exp(jax.random.uniform(jax.random.fold_in(own, axis_at), (shards_of,), jnp.float32, low / len(shards), high / len(shards)))
        factor_of = factor_of * jnp.repeat(draws, extent[axis_at] // shards_of).reshape([-1 if axis == axis_at else 1 for axis in range(len(extent))])
    return factor_of


def bell_draw(own_key, extent, width, most, pieces=(), kind=jnp.bfloat16):
    level = level_of(own_key, extent, pieces, -0.22, 0.18) if pieces else 1.0
    result = jax.random.normal(own_key, extent, jnp.float32) * width * level
    return jnp.minimum(jnp.maximum(result, -most), most).astype(kind)


def setup_inputs(seed: int = 0) -> dict:
    key_of = jax.random.split(jax.random.key(seed), 5)
    tokens = bell_draw(key_of[0], (TOKENS, D), 1.0, 6.0, ((0, 64),))
    gate_weight = bell_draw(key_of[1], (FF, D), D ** -0.5, 0.0625, ((0, 128),))
    up_weight = bell_draw(key_of[2], (FF, D), D ** -0.5, 0.0625, ((0, 128),))
    down_weight = bell_draw(key_of[3], (FF, D), FF ** -0.5, 0.03125, ((0, 128),))
    return {"tokens": tokens, "gate_weight": gate_weight, "up_weight": up_weight, "down_weight": down_weight}


def reference(tokens, gate_weight, up_weight, down_weight):
    gate = jnp.dot(tokens, gate_weight.T, preferred_element_type=jnp.float32)
    up = jnp.dot(tokens, up_weight.T, preferred_element_type=jnp.float32)
    hidden = (jax.nn.silu(gate) * up).astype(jnp.bfloat16)
    return jnp.dot(hidden, down_weight, preferred_element_type=jnp.float32).astype(jnp.bfloat16)
```

```python
import jax
import jax.numpy as jnp
from jax import lax
from jax.sharding import Mesh, PartitionSpec as P

ALL = ("xl", "y", "z", "c", "xh")
CHIPS = ("xl", "y", "z")
BF = jnp.bfloat16
F32 = jnp.float32


def flat(xl, y, z, c, xh):
    return (((xl * 4 + y) * 4 + z) * 2 + c) * 2 + xh


def every():
    for xl in range(2):
        for y in range(4):
            for z in range(4):
                for c in range(2):
                    for xh in range(2):
                        yield xl, y, z, c, xh


def swap_core(v):
    pairs = [(flat(a, y, z, c, h), flat(a, y, z, 1 - c, h)) for a, y, z, c, h in every()]
    return lax.ppermute(v, ALL, pairs)


def swap_far(v):
    pairs = [(flat(a, y, z, c, h), flat(a, y, z, c, 1 - h)) for a, y, z, c, h in every()]
    return lax.ppermute(v, ALL, pairs)


def rows_of(left, weight):
    return lax.dot_general(
        left, weight, (((1,), (1,)), ((), ())), preferred_element_type=F32
    )


def per_device(tokens, gate_weight, up_weight, down_weight):
    d = tokens.shape[1]
    half = d // 2
    c = lax.axis_index("c")
    h = lax.axis_index("xh")
    lo, hi = tokens[:, :half], tokens[:, half:]
    mine = jnp.where(c == 0, lo, hi)
    other = jnp.where(c == 0, hi, lo)
    with jax.named_scope("pre"):
        got = swap_core(other)
    eight = jnp.where(c == 0, jnp.concatenate([mine, got]), jnp.concatenate([got, mine]))
    with jax.named_scope("gather"):
        x_mine = lax.all_to_all(
            jnp.broadcast_to(eight[None], (32, 8, half)), CHIPS, 0, 0, tiled=True
        ).reshape(256, half)
    with jax.named_scope("share"):
        x_got = swap_core(x_mine)
    x = jnp.where(
        c == 0,
        jnp.concatenate([x_mine, x_got], 1),
        jnp.concatenate([x_got, x_mine], 1),
    )
    gate = rows_of(x, gate_weight)
    up = rows_of(x, up_weight)
    hidden = (jax.nn.silu(gate) * up).astype(BF)
    part = jnp.dot(hidden, down_weight, preferred_element_type=F32)
    p_mine = jnp.where(c == 0, part[:, :half], part[:, half:])
    p_other = jnp.where(c == 0, part[:, half:], part[:, :half]).astype(BF)
    with jax.named_scope("fold"):
        p_got = swap_core(p_other)
    total = (p_mine + p_got.astype(F32)).astype(BF)
    with jax.named_scope("scatter"):
        pieces = lax.all_to_all(total.reshape(32, 8, half), CHIPS, 0, 0, tiled=True)
    total = jnp.sum(pieces.astype(F32), axis=0).reshape(2, 2, 2, half)
    keep = jnp.where(h == 0, total[:, 0], total[:, 1])
    send = jnp.where(h == 0, total[:, 1], total[:, 0]).astype(BF)
    with jax.named_scope("far"):
        keep = keep + swap_far(send).astype(F32)
    keep = keep.astype(BF)
    own = jnp.where(c == 0, keep[0], keep[1])
    away = jnp.where(c == 0, keep[1], keep[0])
    with jax.named_scope("post"):
        back = swap_core(away)
    return jnp.where(
        c == 0,
        jnp.concatenate([own, back], 1),
        jnp.concatenate([back, own], 1),
    )


def solution(mesh):
    fine = Mesh(mesh.devices.reshape(2, 4, 4, 2, 2), ALL)
    blk = ("xl", "y", "z", "c")
    return jax.shard_map(
        per_device,
        mesh=fine,
        in_specs=(P(blk, None), P(ALL, None), P(ALL, None), P(ALL, None)),
        out_specs=P(ALL, None),
        check_vma=False,
    )
```

```python
import jax
import jax.numpy as jnp
from jax import lax
from jax.experimental import pallas as pl
from jax.experimental.pallas import tpu as pltpu
from jax.sharding import Mesh, PartitionSpec as P

ALL = ("xl", "y", "z", "c", "xh")
PLANE = ("xl", "y", "z")
CHIPS = ("xl", "y", "z", "xh")
BF = jnp.bfloat16
F32 = jnp.float32


def flat(xl, y, z, c, xh):
    return (((xl * 4 + y) * 4 + z) * 2 + c) * 2 + xh


def every():
    for xl in range(2):
        for y in range(4):
            for z in range(4):
                for c in range(2):
                    for xh in range(2):
                        yield xl, y, z, c, xh


def swap_core(v):
    pairs = [(flat(a, y, z, c, h), flat(a, y, z, 1 - c, h)) for a, y, z, c, h in every()]
    return lax.ppermute(v, ALL, pairs)


def rows_of(left, weight):
    return lax.dot_general(
        left, weight, (((1,), (1,)), ((), ())), preferred_element_type=F32
    )


def hidden_kernel(x_ref, gate_ref, up_ref, hidden_ref):
    x = x_ref[...].reshape(128, x_ref.shape[2])
    gate = rows_of(x, gate_ref[...])
    up = rows_of(x, up_ref[...])
    hidden_ref[...] = (gate / (1.0 + jnp.exp(-gate)) * up).astype(BF)


def down_kernel(hidden_ref, down_ref, out_ref):
    part = jnp.dot(hidden_ref[...], down_ref[...], preferred_element_type=F32)
    out_ref[...] = part.astype(BF).reshape(out_ref.shape)


def fold_kernel(hidden_ref, down_ref, other_ref, out_ref):
    part = jnp.dot(hidden_ref[...], down_ref[...], preferred_element_type=F32)
    other = other_ref[...].reshape(part.shape).astype(F32)
    out_ref[...] = (part + other).astype(BF).reshape(out_ref.shape)


VM = pl.BlockSpec(memory_space=pltpu.VMEM)


def call(kernel, shape, *args):
    return pl.pallas_call(
        kernel,
        out_shape=jax.ShapeDtypeStruct(shape, BF),
        in_specs=[VM] * len(args),
        out_specs=VM,
        compiler_params=pltpu.CompilerParams(vmem_limit_bytes=24 * 2**20),
    )(*args)


def per_device(tokens, gate_weight, up_weight, down_weight):
    rows, d = tokens.shape
    f = gate_weight.shape[0]
    with jax.named_scope("pre"):
        block = swap_core(tokens)
    with jax.named_scope("gather"):
        near = lax.all_to_all(
            jnp.broadcast_to(block[None], (32, rows, d)), PLANE, 0, 0, tiled=True
        )
    with jax.named_scope("share"):
        far = swap_core(near)
    with jax.named_scope("near"):
        hidden = call(hidden_kernel, (128, f), near, gate_weight, up_weight)
        part = call(down_kernel, (64, 2, d), hidden, down_weight)
    with jax.named_scope("fold"):
        part = swap_core(part)
    with jax.named_scope("far"):
        hidden = call(hidden_kernel, (128, f), far, gate_weight, up_weight)
        part = call(fold_kernel, (64, 2, d), hidden, down_weight, part)
    with jax.named_scope("scatter"):
        pieces = lax.all_to_all(part, CHIPS, 0, 0, tiled=True)
    return jnp.sum(pieces.astype(F32), axis=0).astype(BF)


def solution(mesh):
    fine = Mesh(mesh.devices.reshape(2, 4, 4, 2, 2), ALL)
    return jax.shard_map(
        per_device,
        mesh=fine,
        in_specs=(P(("xl", "y", "z", "c"), None), P(ALL, None), P(ALL, None), P(ALL, None)),
        out_specs=P(ALL, None),
        check_vma=False,
    )
```

```python
import jax
import jax.numpy as jnp
from jax import lax
from jax.experimental import pallas as pl
from jax.experimental.pallas import tpu as pltpu
from jax.sharding import Mesh, PartitionSpec as P


ALL = ("xl", "y", "z", "c", "xh")
BF = jnp.bfloat16
F32 = jnp.float32


def move(v, to):
    def flat(x, y, z, c):
        return (((x % 2 * 4 + y) * 4 + z) * 2 + c) * 2 + x // 2

    pairs = []
    for x in range(4):
        for y in range(4):
            for z in range(4):
                for c in range(2):
                    tx, tc = to(x, c)
                    pairs.append((flat(x, y, z, c), flat(tx, y, z, tc)))
    return lax.ppermute(v, ALL, pairs)


def core(v):
    return move(v, lambda x, c: (x, 1 - c))


def inner(v):
    return move(v, lambda x, c: (x ^ 1, c))


def outer(v):
    return move(v, lambda x, c: (3 - x, c))


def rows_of(left, weight):
    return lax.dot_general(
        left, weight, (((1,), (1,)), ((), ())), preferred_element_type=F32
    )


def hidden_kernel(*refs):
    *x_refs, gate_ref, up_ref, hidden_ref = refs
    d = x_refs[0].shape[2]
    x = jnp.concatenate([r[...].reshape(-1, d) for r in x_refs], axis=0)
    gate = rows_of(x, gate_ref[...])
    up = rows_of(x, up_ref[...])
    hidden_ref[...] = (gate / (1.0 + jnp.exp(-gate)) * up).astype(BF)


def down_kernel(at, n_out, *refs):
    hidden_ref, down_ref, *more = refs[:-n_out]
    outs = refs[-n_out:]
    rows = sum(o.shape[0] for o in outs) * 2
    part = jnp.dot(
        hidden_ref[at : at + rows, :], down_ref[...], preferred_element_type=F32
    )
    if more:
        part += more[0][...].reshape(part.shape).astype(F32)
    if more[1:]:
        part += jnp.concatenate(
            [r[...].reshape(rows // 2, -1) for r in more[1:]], axis=0
        ).astype(F32)
    each = rows // n_out
    for i, o in enumerate(outs):
        o[...] = part[i * each : (i + 1) * each].astype(BF).reshape(o.shape)


VM = pl.BlockSpec(memory_space=pltpu.VMEM)


def call(kernel, shapes, *args):
    return pl.pallas_call(
        kernel,
        out_shape=[jax.ShapeDtypeStruct(shape, BF) for shape in shapes],
        in_specs=[VM] * len(args),
        out_specs=[VM] * len(shapes),
        compiler_params=pltpu.CompilerParams(vmem_limit_bytes=20 * 2**20),
    )(*args)


def down(at, shapes, *args):
    return call(lambda *refs: down_kernel(at, len(shapes), *refs), shapes, *args)


def per_device(tokens, *weights):
    rows, d = tokens.shape
    f = weights[0].shape[0]
    block = inner(tokens)
    gate_weight, up_weight, down_weight = weights
    away = lax.all_to_all(
        jnp.broadcast_to(block[None], (16, rows, d)), ("y", "z"), 0, 0, tiled=True
    )
    away_sib = core(away)
    home_a = inner(away[:8])
    home_b = outer(away[8:])
    (hidden,) = call(hidden_kernel, [(128, f)], away, away_sib, gate_weight, up_weight)
    (part,) = down(64, [(32, 2, d)], hidden, down_weight)
    part = core(part)
    part_a, part_b = down(0, [(16, 2, d)] * 2, hidden, down_weight, part)
    back_a = inner(part_a)
    back_b = outer(part_b)
    sib_a = core(home_a)
    sib_b = core(home_b)
    (hidden,) = call(
        hidden_kernel,
        [(128, f)],
        home_a,
        home_b,
        sib_a,
        sib_b,
        gate_weight,
        up_weight,
    )
    (part,) = down(64, [(32, 2, d)], hidden, down_weight)
    part = core(part)
    (part,) = down(
        0, [(32, 2, d)], hidden, down_weight, part, back_a, back_b
    )
    pieces = lax.all_to_all(part, ("y", "z", "xh"), 0, 0, tiled=True)
    return jnp.sum(pieces.astype(F32), axis=0).astype(BF)


def solution(mesh):
    fine = Mesh(mesh.devices.reshape(2, 4, 4, 2, 2), ALL)

    return jax.shard_map(
        per_device,
        mesh=fine,
        in_specs=(P(("xl", "y", "z", "c"), None), P(ALL, None), P(ALL, None), P(ALL, None)),
        out_specs=P(ALL, None),
        check_vma=False,
    )
```

```python
import jax
import jax.numpy as jnp
from jax import lax
from jax.experimental import pallas as pl
from jax.experimental.pallas import tpu as pltpu
from jax.sharding import PartitionSpec as P


ALL = ("blk", "tensor")
BF = jnp.bfloat16
F32 = jnp.float32
R4 = range(4)


def flat(x, y, z, c):
    return ((x % 2 * 4 + y) * 4 + z) * 4 + c * 2 + x // 2


def move(v, to):
    pairs = [
        (flat(x, y, z, c), flat(*to(x, y, z, c)))
        for x in R4
        for y in R4
        for z in R4
        for c in range(2)
    ]
    return lax.ppermute(v, ALL, pairs)


def core(v):
    return move(v, lambda x, y, z, c: (x, y, z, 1 - c))


def ring(v, k):
    return move(
        v,
        lambda x, y, z, c: (x, (y + k) % 4, z, c) if c else (x, y, (z + k) % 4, c),
    )


def near_groups():
    return [
        [
            flat(h * 2 + l, m if c == 0 else s, s if c == 0 else m, c)
            for l in range(2)
            for m in R4
        ]
        for c in range(2)
        for h in range(2)
        for s in R4
    ]


def plane_groups():
    return [
        [
            flat(h * 2 + l, m if c == 0 else s, s if c == 0 else m, c)
            for l in range(2)
            for m in R4
            for h in range(2)
        ]
        for c in range(2)
        for s in R4
    ]


def rows_of(left, weight):
    return lax.dot_general(
        left, weight, (((1,), (1,)), ((), ())), preferred_element_type=F32
    )


def hidden_kernel(*refs):
    *x_refs, gate_ref, up_ref, hidden_ref = refs
    d = x_refs[0].shape[2]
    x = jnp.concatenate([r[...].reshape(-1, d) for r in x_refs], axis=0)
    gate = rows_of(x, gate_ref[...])
    up = rows_of(x, up_ref[...])
    hidden_ref[...] = (gate / (1.0 + jnp.exp(-gate)) * up).astype(BF)


def down_kernel(at, n_out, *refs):
    hidden_ref, down_ref, *more = refs[:-n_out]
    outs = refs[-n_out:]
    rows = sum(o.shape[0] for o in outs) * 2
    part = jnp.dot(
        hidden_ref[at : at + rows, :], down_ref[...], preferred_element_type=F32
    )
    for r in more:
        part += r[...].reshape(part.shape).astype(F32)
    each = rows // n_out
    for i, o in enumerate(outs):
        o[...] = part[i * each : (i + 1) * each].astype(BF).reshape(o.shape)


def add_one_kernel(
    hidden_ref, down_ref, fold_ref, lent_low_ref, lent_high_ref, low_ref, high_ref
):
    rows = hidden_ref.shape[0] // 2
    part = jnp.dot(
        hidden_ref[0:rows, :], down_ref[...], preferred_element_type=F32
    ) + fold_ref[...].reshape(rows, -1).astype(F32)
    each = rows // 2
    half = each // 2
    low, high = part[:each], part[each:]
    low_first = low[:half] + lent_low_ref[...].reshape(half, -1).astype(F32)
    high_last = high[half:] + lent_high_ref[...].reshape(half, -1).astype(F32)
    n = low_ref.shape[0] // 2
    low_ref[0:n] = low_first.astype(BF).reshape(n, 2, -1)
    low_ref[n:] = low[half:].astype(BF).reshape(n, 2, -1)
    high_ref[0:n] = high[:half].astype(BF).reshape(n, 2, -1)
    high_ref[n:] = high_last.astype(BF).reshape(n, 2, -1)


VM = pl.BlockSpec(memory_space=pltpu.VMEM)


def call(kernel, shapes, *args):
    return pl.pallas_call(
        kernel,
        out_shape=[jax.ShapeDtypeStruct(shape, BF) for shape in shapes],
        in_specs=[VM] * len(args),
        out_specs=[VM] * len(shapes),
        compiler_params=pltpu.CompilerParams(vmem_limit_bytes=20 * 2**20),
    )(*args)


def touch_kernel(*refs):
    *weights, out = refs
    out[...] = sum(w[0:8, 0:128].astype(F32) for w in weights)


def touch(*weights):
    return pl.pallas_call(
        touch_kernel,
        out_shape=jax.ShapeDtypeStruct((8, 128), F32),
        in_specs=[VM] * len(weights),
        out_specs=VM,
        compiler_params=pltpu.CompilerParams(
            vmem_limit_bytes=20 * 2**20, has_side_effects=True
        ),
    )(*weights)


def down(at, shapes, *args):
    return call(lambda *refs: down_kernel(at, len(shapes), *refs), shapes, *args)


def per_device(tokens, gate_weight, up_weight, down_weight):
    rows, d = tokens.shape
    f = gate_weight.shape[0]
    block = ring(tokens, 2)
    touch(gate_weight, up_weight)
    two = lax.all_to_all(
        jnp.broadcast_to(block[None], (8, rows, d)),
        ALL,
        0,
        0,
        axis_index_groups=near_groups(),
        tiled=True,
    )
    two_sib = core(two)
    low = ring(two, 1)
    high = ring(two, -1)
    (hidden,) = call(hidden_kernel, [(64, f)], two, two_sib, gate_weight, up_weight)
    (part,) = down(32, [(16, 2, d)], hidden, down_weight)
    part = core(part)
    part_a, part_b = down(0, [(8, 2, d)] * 2, hidden, down_weight, part)
    lent_low = ring(part_a, 1)
    lent_high = ring(part_b, -1)

    low_sib = core(low)
    high_sib = core(high)
    own_a = ring(low[:4], 1)
    own_b = ring(high[4:], -1)
    (hidden,) = call(
        hidden_kernel,
        [(128, f)],
        low,
        high,
        low_sib,
        high_sib,
        gate_weight,
        up_weight,
    )
    (part,) = down(64, [(32, 2, d)], hidden, down_weight)
    part = core(part)
    part_low, part_high = call(
        add_one_kernel,
        [(16, 2, d)] * 2,
        hidden,
        down_weight,
        part,
        lent_low,
        lent_high,
    )
    back_low = ring(part_low, 1)
    back_high = ring(part_high, -1)

    sib_a = core(own_a)
    sib_b = core(own_b)
    (hidden,) = call(
        hidden_kernel,
        [(64, f)],
        own_a,
        own_b,
        sib_a,
        sib_b,
        gate_weight,
        up_weight,
    )
    (part,) = down(32, [(16, 2, d)], hidden, down_weight)
    part = core(part)
    (part,) = down(
        0, [(16, 2, d)], hidden, down_weight, part, back_low, back_high
    )
    pieces = lax.all_to_all(
        part, ALL, 0, 0, axis_index_groups=plane_groups(), tiled=True
    )
    return jnp.sum(pieces.astype(F32), axis=0).astype(BF)


def solution(mesh):
    return jax.shard_map(
        per_device,
        mesh=mesh,
        in_specs=(P("blk", None), P(ALL, None), P(ALL, None), P(ALL, None)),
        out_specs=P(ALL, None),
        check_vma=False,
    )
```

```python
import functools

import jax
import jax.numpy as jnp
from jax import lax
from jax.experimental import pallas as pl
from jax.experimental.pallas import tpu as pltpu
from jax.sharding import PartitionSpec as P


ALL = ("blk", "tensor")
BF = jnp.bfloat16
F32 = jnp.float32
R4 = range(4)


def flat(x, y, z, c):
    return ((x % 2 * 4 + y) * 4 + z) * 4 + c * 2 + x // 2


def move(v, to):
    pairs = [
        (flat(x, y, z, c), flat(*to(x, y, z, c)))
        for x in R4
        for y in R4
        for z in R4
        for c in range(2)
    ]
    return lax.ppermute(v, ALL, pairs)


def core(v):
    return move(v, lambda x, y, z, c: (x, y, z, 1 - c))


def ring(v, k):
    return move(
        v,
        lambda x, y, z, c: (x, (y + k) % 4, z, c) if c else (x, y, (z + k) % 4, c),
    )


def side(v, k):
    return move(
        v,
        lambda x, y, z, c: (x, y, (z + k) % 4, c) if c else (x, (y + k) % 4, z, c),
    )


def first_pair(v):
    here = ring(v, 2)
    there = move(
        v,
        lambda x, y, z, c: (
            (x ^ 1, (y + 2) % 4, z, c) if c else (x ^ 1, y, (z + 2) % 4, c)
        ),
    )
    return here, there


def plane_groups():
    return [
        [
            flat(h * 2 + l, m if c == 0 else s, s if c == 0 else m, c)
            for l in range(2)
            for m in R4
            for h in range(2)
        ]
        for c in range(2)
        for s in R4
    ]


def rows_of(left, weight):
    return lax.dot_general(
        left, weight, (((1,), (1,)), ((), ())), preferred_element_type=F32
    )


def hidden_of(x_refs, gate_ref, up_ref):
    d = x_refs[0].shape[2]
    x = jnp.concatenate([r[...].reshape(-1, d) for r in x_refs], axis=0)
    gate = rows_of(gate_ref[...], x)
    up = rows_of(up_ref[...], x)
    return (gate / (1.0 + jnp.exp(-gate)) * up).T.astype(BF)


def hidden_kernel(*refs):
    *x_refs, gate_ref, up_ref, hidden_ref = refs
    hidden_ref[...] = hidden_of(x_refs, gate_ref, up_ref)


def work_kernel(*refs):
    *x_refs, gate_ref, up_ref, down_ref, sib_ref, own_ref = refs
    down_rows(hidden_of(x_refs, gate_ref, up_ref), down_ref, sib_ref, own_ref)


def down_kernel(hidden_ref, *refs):
    down_rows(hidden_ref[...], *refs)


def down_rows(hidden, down_ref, sib_ref, own_ref):
    part = jnp.dot(hidden, down_ref[...], preferred_element_type=F32)
    rows = own_ref.shape[0]
    own_ref[...] = part[:rows]
    sib_ref[...] = part[rows:].astype(BF).reshape(sib_ref.shape)


def add_kernel(own_ref, fold_ref, *outs):
    d = own_ref.shape[1]
    part = own_ref[...] + fold_ref[...].reshape(-1, d).astype(F32)
    each = part.shape[0] // len(outs)
    for i, o in enumerate(outs):
        o[...] = part[i * each : (i + 1) * each].astype(BF).reshape(o.shape)


def ring_kernel(which, own_ref, fold_ref, lent_ref, out_ref):
    n = out_ref.shape[0]
    d = own_ref.shape[1]
    part = own_ref[2 * n * which : 2 * n * (which + 1), :]
    part += fold_ref[n * which : n * (which + 1)].reshape(-1, d).astype(F32)
    lent = part[n * which : n * (which + 1)] + lent_ref[...].reshape(n, d).astype(F32)
    kept = part[n * (1 - which) : n * (2 - which)]
    h = n // 2
    out_ref[h * which : h * (which + 1)] = lent.astype(BF).reshape(h, 2, d)
    out_ref[h * (1 - which) : h * (2 - which)] = kept.astype(BF).reshape(h, 2, d)


VM = pl.BlockSpec(memory_space=pltpu.VMEM)


def call(kernel, shapes, *args):
    return pl.pallas_call(
        kernel,
        out_shape=shapes,
        in_specs=[VM] * len(args),
        out_specs=[VM] * len(shapes),
        compiler_params=pltpu.CompilerParams(vmem_limit_bytes=12 * 2**20),
    )(*args)


def piece(blocks, d):
    return jax.ShapeDtypeStruct((blocks, 2, d), BF)


def work(weights, *xs):
    d = xs[0].shape[2]
    rows = sum(x.shape[0] * x.shape[1] for x in xs) // 2
    shapes = [piece(rows // 2, d), jax.ShapeDtypeStruct((rows, d), F32)]
    return call(work_kernel, shapes, *xs, *weights)


def add(outs, own, *pieces):
    return call(add_kernel, outs, own, *pieces)


def place_kernel(own_ref, fold_ref, low_ref, high_ref, out_ref):
    me = lax.axis_index("blk")
    own_m = lax.select(me % 2 == 0, me // 8 % 4, me // 2 % 4)
    d = own_ref.shape[1]
    part = own_ref[...]
    for r in (fold_ref, low_ref, high_ref):
        part += r[...].reshape(-1, d).astype(F32)
    for i in range(8):
        m = (own_m + (0, 3, 1, 2)[i // 2]) % 4
        xl = (me // 32 + i % 2) % 2
        out_ref[pl.ds((xl * 4 + m) * 2, 2)] = (
            part[4 * i : 4 * i + 4].astype(BF).reshape(2, 2, d)
        )


def touch_kernel(*refs):
    *weights, out = refs
    out[...] = sum(w[0:8, 0:128].astype(F32) for w in weights)


def touch(*weights):
    return pl.pallas_call(
        touch_kernel,
        out_shape=jax.ShapeDtypeStruct((8, 128), F32),
        in_specs=[VM] * len(weights),
        out_specs=VM,
        compiler_params=pltpu.CompilerParams(
            vmem_limit_bytes=12 * 2**20, has_side_effects=True
        ),
    )(*weights)


def per_device(tokens, gate_weight, up_weight, down_weight):
    rows, d = tokens.shape
    here, there = first_pair(tokens)
    touch(gate_weight)
    touch(up_weight)
    near = jnp.stack([here, there])
    below = side(near, 1)
    above = side(near, -1)
    across = side(near, 2)
    two = jnp.concatenate([near, below, above, across])
    two_sib = core(two)
    low = ring(two, 1)
    high = ring(two, -1)
    weights = (gate_weight, up_weight, down_weight)
    shape = jax.ShapeDtypeStruct((16 * rows, gate_weight.shape[0]), BF)
    (hidden,) = call(hidden_kernel, [shape], two, two_sib, *weights[:2])
    shapes = [piece(16, d), jax.ShapeDtypeStruct((8 * rows, d), F32)]
    part, own_part = call(down_kernel, shapes, hidden, down_weight)
    part = core(part)
    part_a, part_b = add([piece(8, d)] * 2, own_part, part)
    lent_low = ring(part_a, 1)
    lent_high = ring(part_b, -1)

    low_sib = core(low)
    high_sib = core(high)
    own_a = ring(low[:4], 1)
    own_b = ring(high[4:], -1)
    part, own_part = work(weights, low, high, low_sib, high_sib)
    part = core(part)
    (part_low,) = call(
        functools.partial(ring_kernel, 0), [piece(16, d)], own_part, part, lent_low
    )
    back_low = ring(part_low, 1)
    (part_high,) = call(
        functools.partial(ring_kernel, 1), [piece(16, d)], own_part, part, lent_high
    )
    back_high = ring(part_high, -1)

    sib_a = core(own_a)
    sib_b = core(own_b)
    part, own_part = work(weights, own_a, own_b, sib_a, sib_b)
    part = core(part)
    (part,) = call(place_kernel, [piece(16, d)], own_part, part, back_low, back_high)
    pieces = lax.all_to_all(
        part, ALL, 0, 0, axis_index_groups=plane_groups(), tiled=True
    )
    return jnp.sum(pieces.astype(F32), axis=0).astype(BF)


def solution(mesh):
    return jax.shard_map(
        per_device,
        mesh=mesh,
        in_specs=(P("blk", None), P(ALL, None), P(ALL, None), P(ALL, None)),
        out_specs=P(ALL, None),
        check_vma=False,
    )
```

```python
import functools

import jax
import jax.numpy as jnp
from jax import lax
from jax.experimental import pallas as pl
from jax.experimental.pallas import tpu as pltpu
from jax.sharding import PartitionSpec as P


ALL = ("blk", "tensor")
BF = jnp.bfloat16
F32 = jnp.float32
R4 = range(4)


def flat(x, y, z, c):
    return ((x % 2 * 4 + y) * 4 + z) * 4 + c * 2 + x // 2


def move(v, to):
    pairs = [
        (flat(x, y, z, c), flat(*to(x, y, z, c)))
        for x in R4
        for y in R4
        for z in R4
        for c in range(2)
    ]
    return lax.ppermute(v, ALL, pairs)


def core(v):
    return move(v, lambda x, y, z, c: (x, y, z, 1 - c))


def ring(v, k):
    return move(
        v,
        lambda x, y, z, c: (x, (y + k) % 4, z, c) if c else (x, y, (z + k) % 4, c),
    )


def side(v, k):
    return move(
        v,
        lambda x, y, z, c: (x, y, (z + k) % 4, c) if c else (x, (y + k) % 4, z, c),
    )


def first_pair(v):
    here = ring(v, 2)
    there = move(
        v,
        lambda x, y, z, c: (
            (x ^ 1, (y + 2) % 4, z, c) if c else (x ^ 1, y, (z + 2) % 4, c)
        ),
    )
    return here, there


def plane_groups():
    return [
        [
            flat(h * 2 + l, m if c == 0 else s, s if c == 0 else m, c)
            for l in range(2)
            for m in R4
            for h in range(2)
        ]
        for c in range(2)
        for s in R4
    ]


def rows_of(left, weight):
    return lax.dot_general(
        left, weight, (((1,), (1,)), ((), ())), preferred_element_type=F32
    )


def hidden_of(x_refs, gate_ref, up_ref):
    d = x_refs[0].shape[2]
    x = jnp.concatenate([r[...].reshape(-1, d) for r in x_refs], axis=0)
    gate = rows_of(gate_ref[...], x)
    up = rows_of(up_ref[...], x)
    return (gate / (1.0 + jnp.exp(-gate)) * up).T.astype(BF)


def hidden_kernel(*refs):
    *x_refs, gate_ref, up_ref, hidden_ref = refs
    hidden_ref[...] = hidden_of(x_refs, gate_ref, up_ref)


def work_kernel(pieces, *refs):
    *x_refs, gate_ref, up_ref, down_ref = refs[: -pieces - 1]
    hidden = hidden_of(x_refs, gate_ref, up_ref)
    down_rows(hidden, down_ref, *refs[-pieces - 1 :])


def down_kernel(hidden_ref, *refs):
    down_rows(hidden_ref[...], *refs)


def down_rows(hidden, down_ref, *outs):
    part = jnp.dot(hidden, down_ref[...], preferred_element_type=F32)
    *sib_refs, own_ref = outs
    at = own_ref.shape[0]
    own_ref[...] = part[:at]
    for sib_ref in sib_refs:
        rows = sib_ref.shape[0] * 2
        sib_ref[...] = part[at : at + rows].astype(BF).reshape(sib_ref.shape)
        at += rows


def add_kernel(own_ref, fold_ref, *outs):
    d = own_ref.shape[1]
    part = own_ref[...] + fold_ref[...].reshape(-1, d).astype(F32)
    each = part.shape[0] // len(outs)
    for i, o in enumerate(outs):
        o[...] = part[i * each : (i + 1) * each].astype(BF).reshape(o.shape)


def ring_kernel(which, own_ref, fold_ref, lent_ref, out_ref):
    n = out_ref.shape[0]
    d = own_ref.shape[1]
    part = own_ref[2 * n * which : 2 * n * (which + 1), :]
    part += fold_ref[...].reshape(-1, d).astype(F32)
    lent = part[n * which : n * (which + 1)] + lent_ref[...].reshape(n, d).astype(F32)
    kept = part[n * (1 - which) : n * (2 - which)]
    h = n // 2
    out_ref[h * which : h * (which + 1)] = lent.astype(BF).reshape(h, 2, d)
    out_ref[h * (1 - which) : h * (2 - which)] = kept.astype(BF).reshape(h, 2, d)


VM = pl.BlockSpec(memory_space=pltpu.VMEM)


def call(kernel, shapes, *args):
    return pl.pallas_call(
        kernel,
        out_shape=shapes,
        in_specs=[VM] * len(args),
        out_specs=[VM] * len(shapes),
        compiler_params=pltpu.CompilerParams(vmem_limit_bytes=12 * 2**20),
    )(*args)


def piece(blocks, d):
    return jax.ShapeDtypeStruct((blocks, 2, d), BF)


def work(weights, *xs, pieces=1):
    d = xs[0].shape[2]
    rows = sum(x.shape[0] * x.shape[1] for x in xs) // 2
    shapes = [piece(rows // 2 // pieces, d)] * pieces
    shapes.append(jax.ShapeDtypeStruct((rows, d), F32))
    return call(functools.partial(work_kernel, pieces), shapes, *xs, *weights)


def add(outs, own, *pieces):
    return call(add_kernel, outs, own, *pieces)


def place_kernel(own_ref, fold_ref, low_ref, high_ref, out_ref):
    me = lax.axis_index("blk")
    own_m = lax.select(me % 2 == 0, me // 8 % 4, me // 2 % 4)
    d = own_ref.shape[1]
    part = own_ref[...]
    for r in (fold_ref, low_ref, high_ref):
        part += r[...].reshape(-1, d).astype(F32)
    for i in range(8):
        m = (own_m + (0, 3, 1, 2)[i // 2]) % 4
        xl = (me // 32 + i % 2) % 2
        out_ref[pl.ds((xl * 4 + m) * 2, 2)] = (
            part[4 * i : 4 * i + 4].astype(BF).reshape(2, 2, d)
        )


def touch_kernel(*refs):
    *weights, out = refs
    out[...] = sum(w[0:8, 0:128].astype(F32) for w in weights)


def touch(*weights):
    return pl.pallas_call(
        touch_kernel,
        out_shape=jax.ShapeDtypeStruct((8, 128), F32),
        in_specs=[VM] * len(weights),
        out_specs=VM,
        compiler_params=pltpu.CompilerParams(
            vmem_limit_bytes=12 * 2**20, has_side_effects=True
        ),
    )(*weights)


def per_device(tokens, gate_weight, up_weight, down_weight):
    rows, d = tokens.shape
    here, there = first_pair(tokens)
    touch(gate_weight)
    touch(up_weight)
    near = jnp.stack([here, there])
    below = side(near, 1)
    above = side(near, -1)
    across = side(near, 2)
    two = jnp.concatenate([near, below, above, across])
    two_sib = core(two)
    low = ring(two, 1)
    high = ring(two, -1)
    weights = (gate_weight, up_weight, down_weight)
    shape = jax.ShapeDtypeStruct((16 * rows, gate_weight.shape[0]), BF)
    (hidden,) = call(hidden_kernel, [shape], two, two_sib, *weights[:2])
    shapes = [piece(16, d), jax.ShapeDtypeStruct((8 * rows, d), F32)]
    part, own_part = call(down_kernel, shapes, hidden, down_weight)
    part = core(part)
    part_a, part_b = add([piece(8, d)] * 2, own_part, part)
    lent_low = ring(part_a, 1)
    lent_high = ring(part_b, -1)

    low_sib = core(low)
    high_sib = core(high)
    own_a = ring(low[:4], 1)
    own_b = ring(high[4:], -1)
    for_low, for_high, own_part = work(weights, low, high, low_sib, high_sib, pieces=2)
    fold_low = core(for_low)
    fold_high = core(for_high)
    (part_low,) = call(
        functools.partial(ring_kernel, 0), [piece(16, d)], own_part, fold_low, lent_low
    )
    back_low = ring(part_low, 1)
    (part_high,) = call(
        functools.partial(ring_kernel, 1), [piece(16, d)], own_part, fold_high, lent_high
    )
    back_high = ring(part_high, -1)

    sib_a = core(own_a)
    sib_b = core(own_b)
    part, own_part = work(weights, own_a, own_b, sib_a, sib_b)
    part = core(part)
    (part,) = call(place_kernel, [piece(16, d)], own_part, part, back_low, back_high)
    pieces = lax.all_to_all(
        part, ALL, 0, 0, axis_index_groups=plane_groups(), tiled=True
    )
    return jnp.sum(pieces.astype(F32), axis=0).astype(BF)


def solution(mesh):
    return jax.shard_map(
        per_device,
        mesh=mesh,
        in_specs=(P("blk", None), P(ALL, None), P(ALL, None), P(ALL, None)),
        out_specs=P(ALL, None),
        check_vma=False,
    )
```
